16 devices in a mesh: dp: 2 (over y, z), sp: 8 (over x, core).
Axes of the slice: x: 4, y: 2, z: 1, core: 2. Of those that a mesh axis runs over, the one named last changes fastest.
The devices are a block of a 4x4x8 slice.
Arguments:
- x_in: bfloat16 [8, 4096, 2304], P('dp', 'sp'), parts along dimension 0
- dy_in: bfloat16 [8, 4096, 2304], P('dp', 'sp'), parts along dimension 0
- positions: int32 [8192], P(('dp', 'sp')), parts along dimension 0
- w_q: bfloat16 [2304, 2048], replicated
- w_k: bfloat16 [2304, 1024], replicated
- w_v: bfloat16 [2304, 1024], replicated
- w_o: bfloat16 [2048, 2304], replicated
- w_pre: float32 [2304], replicated
- w_post: float32 [2304], replicated
- q_norm: float32 [256], replicated
- k_norm: float32 [256], replicated
Outputs:
- output 1: bfloat16 [8, 4096, 2304], P('dp', 'sp'), parts along dimension 0
- output 2: bfloat16 [8, 4096, 2304], P('dp', 'sp'), parts along dimension 0
- output 3: bfloat16 [4608, 2048], P('dp'), parts along dimension 0
- output 4: bfloat16 [4608, 1024], P('dp'), parts along dimension 0
- output 5: bfloat16 [4608, 1024], P('dp'), parts along dimension 0
- output 6: bfloat16 [4096, 2304], P('dp'), parts along dimension 0
- output 7: float32 [4608], P('dp'), parts along dimension 0
- output 8: float32 [4608], P('dp'), parts along dimension 0
- output 9: float32 [512], P('dp'), parts along dimension 0
- output 10: float32 [512], P('dp'), parts along dimension 0
There are 2 independent parts. The reference program is written for one: setup_inputs(seed, part) draws one part's arguments, and reference() takes and returns one part's arrays. A program takes and returns all parts, laid end to end along the dimension named above; an argument that names none is the same for every part.
All inputs are finite; a program needn't handle non-finite values.
Results may differ from the reference program's by a relative error of at most 0.02.
Values are sent between devices in bfloat16 or wider.
A program may use at most 768 MiB of HBM per device.

```python
import functools
import jax
import jax.numpy as jnp
from jax import lax

B = 4
SEQ = 4096
D = 2304
H = 8
K = 4
HEAD = 256

EPS = 1e-6
ROPE_BASE = 1000000.0
ROPE_SCALE = 8.0
NEG_BIG = -1e30
Q_ROWS = min(128, SEQ)


def setup_inputs(seed: int = 0, part: int = 0) -> dict:
    base_key = jax.random.key(seed)
    own = jax.random.split(jax.random.fold_in(base_key, part), 4)
    shared = jax.random.split(base_key, 8)
    x_in = jax.random.normal(own[0], (B, SEQ, D), jnp.float32).astype(jnp.bfloat16)
    dy_in = jax.random.normal(own[1], (B, SEQ, D), jnp.float32).astype(jnp.bfloat16)
    start = jax.random.randint(own[2], (1,), 0, 1000)
    gaps = jax.random.randint(own[3], (SEQ,), 1, 5)
    positions = (start + jnp.cumsum(gaps) - gaps[0]).astype(jnp.int32)
    w_q = (jax.random.normal(shared[0], (D, H * HEAD), jnp.float32) * D ** -0.5).astype(jnp.bfloat16)
    w_k = (jax.random.normal(shared[1], (D, K * HEAD), jnp.float32) * D ** -0.5).astype(jnp.bfloat16)
    w_v = (jax.random.normal(shared[2], (D, K * HEAD), jnp.float32) * D ** -0.5).astype(jnp.bfloat16)
    w_o = (jax.random.normal(shared[3], (H * HEAD, D), jnp.float32) * (H * HEAD) ** -0.5).astype(jnp.bfloat16)
    w_pre = 0.3 * jax.random.normal(shared[4], (D,), jnp.float32)
    w_post = 0.3 * jax.random.normal(shared[5], (D,), jnp.float32)
    q_norm = 0.3 + 0.3 * jax.random.normal(shared[6], (HEAD,), jnp.float32)
    k_norm = 0.3 + 0.3 * jax.random.normal(shared[7], (HEAD,), jnp.float32)
    return {'x_in': x_in, 'dy_in': dy_in, 'positions': positions, 'w_q': w_q, 'w_k': w_k, 'w_v': w_v, 'w_o': w_o, 'w_pre': w_pre, 'w_post': w_post, 'q_norm': q_norm, 'k_norm': k_norm}


def rms_scale(x_f32, weight):
    inv_rms = lax.rsqrt(jnp.mean(x_f32 * x_f32, axis=-1, keepdims=True) + EPS)
    return x_f32 * inv_rms * (1.0 + weight)


def norm_rope(heads_f32, weight, cosines, sines):
    half_dim = HEAD // 2
    normed = rms_scale(heads_f32, weight)
    first = normed[..., :half_dim]
    second = normed[..., half_dim:]
    cos_b = cosines[None, :, None, :]
    sin_b = sines[None, :, None, :]
    return jnp.concatenate([first * cos_b - second * sin_b, second * cos_b + first * sin_b], axis=-1)


def attention(q_rot, k_rot, v_heads):
    group = H // K
    blocks = SEQ // Q_ROWS
    q_blocks = jnp.moveaxis(q_rot.reshape(B, blocks, Q_ROWS, K, group, HEAD), 1, 0)
    key_f32 = k_rot.astype(jnp.float32)
    val_f32 = v_heads.astype(jnp.float32)
    col_ids = jnp.arange(SEQ)

    def one_block(item):
        q_blk, index = item
        scores = jnp.einsum('bqkgh,bskh->bkgqs', q_blk.astype(jnp.float32), key_f32) * HEAD ** -0.5
        row_ids = index * Q_ROWS + jnp.arange(Q_ROWS)
        scores = jnp.where(row_ids[:, None] >= col_ids[None, :], scores, NEG_BIG)
        attn_prob = jax.nn.softmax(scores, axis=-1).astype(jnp.bfloat16).astype(jnp.float32)
        return jnp.einsum('bkgqs,bskh->bqkgh', attn_prob, val_f32).astype(jnp.bfloat16)

    block_out = lax.map(jax.checkpoint(one_block), (q_blocks, jnp.arange(blocks)))
    return jnp.moveaxis(block_out, 0, 1).reshape(B, SEQ, H, HEAD)


def forward(positions, x_in, w_q, w_k, w_v, w_o, w_pre, w_post, q_norm, k_norm):
    x_f32 = x_in.astype(jnp.float32)
    normed = rms_scale(x_f32, w_pre).astype(jnp.bfloat16).astype(jnp.float32)
    q_proj = jnp.einsum('bsd,dn->bsn', normed, w_q.astype(jnp.float32)).astype(jnp.bfloat16)
    k_proj = jnp.einsum('bsd,dn->bsn', normed, w_k.astype(jnp.float32)).astype(jnp.bfloat16)
    v_proj = jnp.einsum('bsd,dn->bsn', normed, w_v.astype(jnp.float32)).astype(jnp.bfloat16)
    half_dim = HEAD // 2
    inv_freq = ROPE_BASE ** (-jnp.arange(half_dim, dtype=jnp.float32) * 2.0 / HEAD)
    angles = (positions.astype(jnp.float32) / ROPE_SCALE)[:, None] * inv_freq[None, :]
    cosines = jnp.cos(angles)
    sines = jnp.sin(angles)
    q_rot = norm_rope(q_proj.reshape(B, SEQ, H, HEAD).astype(jnp.float32), q_norm, cosines, sines).astype(jnp.bfloat16)
    k_rot = norm_rope(k_proj.reshape(B, SEQ, K, HEAD).astype(jnp.float32), k_norm, cosines, sines).astype(jnp.bfloat16)
    v_heads = v_proj.reshape(B, SEQ, K, HEAD)
    attn_out = attention(q_rot, k_rot, v_heads)
    proj = jnp.einsum('bsn,nd->bsd', attn_out.reshape(B, SEQ, H * HEAD).astype(jnp.float32), w_o.astype(jnp.float32)).astype(jnp.bfloat16)
    return (x_f32 + rms_scale(proj.astype(jnp.float32), w_post)).astype(jnp.bfloat16)


def reference(x_in, dy_in, positions, w_q, w_k, w_v, w_o, w_pre, w_post, q_norm, k_norm):
    y_out, pullback = jax.vjp(functools.partial(forward, positions), x_in, w_q, w_k, w_v, w_o, w_pre, w_post, q_norm, k_norm)
    grads = pullback(dy_in)
    return (y_out, grads[0], grads[1], grads[2], grads[3], grads[4], grads[5], grads[6], grads[7], grads[8])
```

```python
import functools
import jax
import jax.numpy as jnp
from jax import lax
from jax.experimental import pallas as pl
from jax.experimental.pallas import tpu as pltpu
from jax.sharding import PartitionSpec as P

EPS = 1e-6
ROPE_BASE = 1000000.0
ROPE_SCALE = 8.0
NEG_BIG = -1e30
VMEM_LIMIT = 56 * 1024 * 1024
F32 = jnp.float32
BF16 = jnp.bfloat16


def rms_scale(x_f32, weight):
    inv_rms = lax.rsqrt(jnp.mean(x_f32 * x_f32, axis=-1, keepdims=True) + EPS)
    return x_f32 * inv_rms * (1.0 + weight)


def pre_norm(x_f32, weight):
    return rms_scale(x_f32, weight).astype(BF16)


def post_norm(proj, weight):
    return rms_scale(proj.astype(F32), weight)


def rope_tables(positions, head):
    half_dim = head // 2
    inv_freq = ROPE_BASE ** (-jnp.arange(half_dim, dtype=F32) * 2.0 / head)
    angles = (positions.astype(F32) / ROPE_SCALE)[:, None] * inv_freq[None, :]
    return jnp.cos(angles), jnp.sin(angles)


def params(ndim):
    return pltpu.CompilerParams(dimension_semantics=("arbitrary",) * ndim, vmem_limit_bytes=VMEM_LIMIT)


def cost(flops, nbytes):
    return pl.CostEstimate(flops=int(flops), bytes_accessed=int(nbytes), transcendentals=0)


def rotate(x, scale1, cosines, sines):
    half = x.shape[-1] // 2
    inv = lax.rsqrt(jnp.mean(x * x, axis=-1, keepdims=True) + EPS)
    normed = x * inv * scale1
    first, second = normed[:, :half], normed[:, half:]
    return jnp.concatenate([first * cosines - second * sines, second * cosines + first * sines], axis=-1)


def unrotate(dy, x, scale1, cosines, sines):
    half = x.shape[-1] // 2
    inv = lax.rsqrt(jnp.mean(x * x, axis=-1, keepdims=True) + EPS)
    unit = x * inv
    d1, d2 = dy[:, :half], dy[:, half:]
    dn = jnp.concatenate([d1 * cosines + d2 * sines, d2 * cosines - d1 * sines], axis=-1)
    du = dn * scale1
    dx = inv * (du - unit * jnp.mean(du * unit, axis=-1, keepdims=True))
    return dx, jnp.sum(dn * unit, axis=0, keepdims=True)


def packed_spec(tokens, lanes, rep, part, offset=0):
    return pl.BlockSpec((None, None, tokens, lanes), lambda k, b: (k * rep + b // part, b % part, 0, offset))


def flat_spec(tokens, lanes, offset=0):
    return pl.BlockSpec((None, tokens, lanes), lambda k, b: (b, 0, k + offset))


def whole_spec(shape):
    return pl.BlockSpec(shape, lambda k, b: (0,) * len(shape))


def q_pack(q_proj, norm, cosines, sines, head, kv_heads, rep):
    batch, tokens, wide = q_proj.shape
    lanes = wide // kv_heads
    part = batch // rep

    def body(x_ref, w_ref, c_ref, s_ref, o_ref):
        for g in range(lanes // head):
            cols = slice(g * head, (g + 1) * head)
            out = rotate(x_ref[:, cols].astype(F32), 1.0 + w_ref[...], c_ref[...], s_ref[...]).astype(BF16)
            o_ref[:, cols] = (out.astype(F32) * head ** -0.5).astype(BF16)

    return pl.pallas_call(
        body, grid=(kv_heads, batch),
        in_specs=[flat_spec(tokens, lanes), whole_spec((1, head)), whole_spec(cosines.shape), whole_spec(sines.shape)],
        out_specs=packed_spec(tokens, lanes, rep, part),
        out_shape=jax.ShapeDtypeStruct((kv_heads * rep, part, tokens, lanes), BF16),
        compiler_params=params(2), cost_estimate=cost(20 * q_proj.size, 4 * q_proj.size), name='q_pack',
    )(q_proj, norm.reshape(1, head), cosines, sines)


def kv_pack(kv_proj, norm, cosines, sines, head, kv_heads, rep):
    batch, tokens, _ = kv_proj.shape
    part = batch // rep

    def body(k_ref, v_ref, w_ref, c_ref, s_ref, o_ref):
        o_ref[:, :head] = rotate(k_ref[...].astype(F32), 1.0 + w_ref[...], c_ref[...], s_ref[...]).astype(BF16)
        o_ref[:, head:] = v_ref[...]

    return pl.pallas_call(
        body, grid=(kv_heads, batch),
        in_specs=[flat_spec(tokens, head), flat_spec(tokens, head, kv_heads), whole_spec((1, head)),
                  whole_spec(cosines.shape), whole_spec(sines.shape)],
        out_specs=packed_spec(tokens, 2 * head, rep, part),
        out_shape=jax.ShapeDtypeStruct((kv_heads * rep, part, tokens, 2 * head), BF16),
        compiler_params=params(2), cost_estimate=cost(10 * kv_proj.size, 4 * kv_proj.size), name='kv_pack',
    )(kv_proj, kv_proj, norm.reshape(1, head), cosines, sines)


def copy_body(i_ref, o_ref):
    o_ref[...] = i_ref[...]


def pack(flat, kv_heads, rep):
    batch, tokens, wide = flat.shape
    lanes = wide // kv_heads
    part = batch // rep
    return pl.pallas_call(
        copy_body, grid=(kv_heads, batch),
        in_specs=[flat_spec(tokens, lanes)], out_specs=packed_spec(tokens, lanes, rep, part),
        out_shape=jax.ShapeDtypeStruct((kv_heads * rep, part, tokens, lanes), flat.dtype),
        compiler_params=params(2), cost_estimate=cost(2 * flat.size, 4 * flat.size), name='pack',
    )(flat)


def unpack(packed, kv_heads, rep):
    _, part, tokens, lanes = packed.shape
    batch = part * rep
    return pl.pallas_call(
        copy_body, grid=(kv_heads, batch),
        in_specs=[packed_spec(tokens, lanes, rep, part)], out_specs=flat_spec(tokens, lanes),
        out_shape=jax.ShapeDtypeStruct((batch, tokens, kv_heads * lanes), packed.dtype),
        compiler_params=params(2), cost_estimate=cost(2 * packed.size, 4 * packed.size), name='unpack',
    )(packed)


def first_step():
    return jnp.logical_and(pl.program_id(0) == 0, pl.program_id(1) == 0)


def q_unpack(dq, q_proj, norm, cosines, sines, head, kv_heads, rep):
    batch, tokens, wide = q_proj.shape
    lanes = wide // kv_heads
    part = batch // rep

    def body(d_ref, x_ref, w_ref, c_ref, s_ref, o_ref, n_ref):
        @pl.when(first_step())
        def _():
            n_ref[...] = jnp.zeros_like(n_ref)
        for g in range(lanes // head):
            cols = slice(g * head, (g + 1) * head)
            dx, dn = unrotate(d_ref[:, cols].astype(F32), x_ref[:, cols].astype(F32), 1.0 + w_ref[...], c_ref[...], s_ref[...])
            o_ref[:, cols] = dx.astype(BF16)
            n_ref[...] += dn

    return pl.pallas_call(
        body, grid=(kv_heads, batch),
        in_specs=[packed_spec(tokens, lanes, rep, part), flat_spec(tokens, lanes), whole_spec((1, head)),
                  whole_spec(cosines.shape), whole_spec(sines.shape)],
        out_specs=(flat_spec(tokens, lanes), whole_spec((1, head))),
        out_shape=(jax.ShapeDtypeStruct(q_proj.shape, BF16), jax.ShapeDtypeStruct((1, head), F32)),
        compiler_params=params(2), cost_estimate=cost(30 * q_proj.size, 6 * q_proj.size), name='q_unpack',
    )(dq, q_proj, norm.reshape(1, head), cosines, sines)


def kv_unpack(dkv, kv_proj, norm, cosines, sines, head, kv_heads, rep):
    batch, tokens, wide = kv_proj.shape
    part = batch // rep

    def body(d_ref, x_ref, w_ref, c_ref, s_ref, k_ref, v_ref, n_ref):
        @pl.when(first_step())
        def _():
            n_ref[...] = jnp.zeros_like(n_ref)
        dx, dn = unrotate(d_ref[:, :head].astype(F32), x_ref[...].astype(F32), 1.0 + w_ref[...], c_ref[...], s_ref[...])
        k_ref[...] = dx.astype(BF16)
        v_ref[...] = d_ref[:, head:]
        n_ref[...] += dn

    half = jax.ShapeDtypeStruct((batch, tokens, wide // 2), BF16)
    return pl.pallas_call(
        body, grid=(kv_heads, batch),
        in_specs=[packed_spec(tokens, 2 * head, rep, part, 1), flat_spec(tokens, head), whole_spec((1, head)),
                  whole_spec(cosines.shape), whole_spec(sines.shape)],
        out_specs=(flat_spec(tokens, head), flat_spec(tokens, head), whole_spec((1, head))),
        out_shape=(half, half, jax.ShapeDtypeStruct((1, head), F32)),
        compiler_params=params(2), cost_estimate=cost(15 * kv_proj.size, 6 * kv_proj.size), name='kv_unpack',
    )(dkv, kv_proj, norm.reshape(1, head), cosines, sines)


NT = (((1,), (1,)), ((), ()))
TN = (((0,), (0,)), ((), ()))
NN = (((1,), (0,)), ((), ()))


def dot(a, b, dims):
    return lax.dot_general(a, b, dims, preferred_element_type=F32)


def to_row(column):
    return jnp.broadcast_to(column, (column.shape[0], 128)).T[:8, :]


def attention_fwd(q, kv, head):
    slots, part, tokens, lanes = q.shape
    per_kv = lanes // head

    def body(q_ref, kv_ref, o_ref, lse_ref, m_sc, l_sc, acc_sc):
        qi = pl.program_id(1)
        m_sc[...] = jnp.full_like(m_sc, NEG_BIG)
        l_sc[...] = jnp.zeros_like(l_sc)
        acc_sc[...] = jnp.zeros_like(acc_sc)

        def step(kj, masked):
            k = kv_ref[kj, :, :head]
            v = kv_ref[kj, :, head:]
            for g in range(per_kv):
                s = dot(q_ref[:, g * head:(g + 1) * head], k, NT)
                if masked:
                    rows = lax.broadcasted_iota(jnp.int32, s.shape, 0)
                    cols = lax.broadcasted_iota(jnp.int32, s.shape, 1)
                    s = jnp.where(rows >= cols, s, NEG_BIG)
                m_old = m_sc[g]
                m_new = jnp.maximum(m_old, jnp.max(s, axis=-1, keepdims=True))
                p = jnp.exp(s - m_new[:, :1])
                fade = jnp.exp(m_old - m_new)
                l_sc[g] = l_sc[g] * fade + jnp.sum(p, axis=-1, keepdims=True)
                acc_sc[g] = acc_sc[g] * fade[:, :1] + dot(p.astype(BF16), v, NN)
                m_sc[g] = m_new

        def loop_body(kj, carry):
            step(kj, False)
            return carry

        lax.fori_loop(0, qi, loop_body, 0)
        step(qi, True)
        for g in range(per_kv):
            o_ref[:, g * head:(g + 1) * head] = (acc_sc[g] / l_sc[g][:, :1]).astype(BF16)
            lse_ref[g * 8:(g + 1) * 8, :] = (m_sc[g] + jnp.log(l_sc[g])).T[:8, :]

    pairs = part * per_kv * (slots * tokens) ** 2 // 2
    return pl.pallas_call(
        body, grid=(part, slots),
        in_specs=[pl.BlockSpec((None, None, tokens, lanes), lambda b, i: (i, b, 0, 0)),
                  pl.BlockSpec((slots, None, tokens, 2 * head), lambda b, i: (0, b, 0, 0))],
        out_specs=(pl.BlockSpec((None, None, tokens, lanes), lambda b, i: (i, b, 0, 0)),
                   pl.BlockSpec((None, None, per_kv * 8, tokens), lambda b, i: (i, b, 0, 0))),
        out_shape=(jax.ShapeDtypeStruct(q.shape, BF16), jax.ShapeDtypeStruct((slots, part, per_kv * 8, tokens), F32)),
        scratch_shapes=[pltpu.VMEM((per_kv, tokens, 128), F32), pltpu.VMEM((per_kv, tokens, 128), F32),
                        pltpu.VMEM((per_kv, tokens, head), F32)],
        compiler_params=params(2), cost_estimate=cost(8 * pairs * head, 8 * q.size), name='attention_fwd',
    )(q, kv)


def row_dots(o, d_o, head):
    slots, part, tokens, lanes = o.shape
    per_kv = lanes // head

    def body(o_ref, d_ref, out_ref):
        for g in range(per_kv):
            cols = slice(g * head, (g + 1) * head)
            total = jnp.sum(o_ref[:, cols].astype(F32) * d_ref[:, cols].astype(F32), axis=-1, keepdims=True)
            out_ref[g * 8:(g + 1) * 8, :] = to_row(total)

    spec = pl.BlockSpec((None, None, tokens, lanes), lambda b, i: (i, b, 0, 0))
    return pl.pallas_call(
        body, grid=(part, slots), in_specs=[spec, spec],
        out_specs=pl.BlockSpec((None, None, per_kv * 8, tokens), lambda b, i: (i, b, 0, 0)),
        out_shape=jax.ShapeDtypeStruct((slots, part, per_kv * 8, tokens), F32),
        compiler_params=params(2), cost_estimate=cost(4 * o.size, 4 * o.size), name='row_dots',
    )(o, d_o)


def attention_bwd(q, kv, d_o, lse, delta, head):
    slots, part, tokens, lanes = q.shape
    per_kv = lanes // head

    def body(q_ref, kv_ref, d_ref, lse_ref, delta_ref, out_ref, dq_sc, dk_sc, dv_sc):
        kj = pl.program_id(1)
        dk_sc[...] = jnp.zeros_like(dk_sc)
        dv_sc[...] = jnp.zeros_like(dv_sc)

        @pl.when(kj == 0)
        def _():
            dq_sc[...] = jnp.zeros_like(dq_sc)

        def step(qi, masked):
            k = kv_ref[:, :head]
            v = kv_ref[:, head:]
            for g in range(per_kv):
                cols = slice(g * head, (g + 1) * head)
                q_g = q_ref[qi, :, cols]
                d_g = d_ref[qi, :, cols]
                s = dot(k, q_g, NT)
                if masked:
                    key_ids = lax.broadcasted_iota(jnp.int32, s.shape, 0)
                    row_ids = lax.broadcasted_iota(jnp.int32, s.shape, 1)
                    s = jnp.where(row_ids >= key_ids, s, NEG_BIG)
                p = jnp.exp(s - lse_ref[qi, g * 8:g * 8 + 1, :])
                dp = dot(v, d_g, NT)
                ds = (p * (dp - delta_ref[qi, g * 8:g * 8 + 1, :])).astype(BF16)
                dv_sc[...] += dot(p.astype(BF16), d_g, NN)
                dk_sc[...] += dot(ds, q_g, NN)
                dq_sc[qi, :, cols] += dot(ds, k, TN)

        def loop_body(qi, carry):
            step(qi, False)
            return carry

        step(kj, True)
        lax.fori_loop(kj + 1, slots, loop_body, 0)
        out_ref[:, :lanes] = (dq_sc[kj] * head ** -0.5).astype(BF16)
        out_ref[:, lanes:lanes + head] = dk_sc[...].astype(BF16)
        out_ref[:, lanes + head:] = dv_sc[...].astype(BF16)

    pairs = part * per_kv * (slots * tokens) ** 2 // 2
    wide = lanes + 2 * head
    kv_block = pl.BlockSpec((None, None, tokens, 2 * head), lambda b, j: (j, b, 0, 0))
    every = pl.BlockSpec((slots, None, tokens, lanes), lambda b, j: (0, b, 0, 0))
    rows = pl.BlockSpec((slots, None, per_kv * 8, tokens), lambda b, j: (0, b, 0, 0))
    return pl.pallas_call(
        body, grid=(part, slots),
        in_specs=[every, kv_block, every, rows, rows],
        out_specs=pl.BlockSpec((None, None, tokens, wide), lambda b, j: (j, b, 0, 0)),
        out_shape=jax.ShapeDtypeStruct((slots, part, tokens, wide), BF16),
        scratch_shapes=[pltpu.VMEM((slots, tokens, lanes), F32), pltpu.VMEM((tokens, head), F32), pltpu.VMEM((tokens, head), F32)],
        compiler_params=params(2), cost_estimate=cost(20 * pairs * head, 12 * q.size), name='attention_bwd',
    )(q, kv, d_o, lse, delta)


def solution(mesh):
    group = mesh.shape['sp']

    def exchange(arr):
        return lax.all_to_all(arr, 'sp', 0, 0, tiled=True)

    def scatter(grad):
        return lax.psum_scatter(grad, 'sp', scatter_dimension=0, tiled=True).astype(BF16)

    def gather(piece):
        return lax.all_gather(piece, 'sp', axis=0, tiled=True)

    def device_step(x_in, dy_in, positions, w_q, w_k, w_v, w_o, w_pre, w_post, q_norm, k_norm):
        head = q_norm.shape[0]
        kv_heads = w_k.shape[1] // head
        rep = group // kv_heads
        assert rep * kv_heads == group and x_in.shape[0] % rep == 0
        assert w_q.shape[1] == 2 * w_k.shape[1]
        w_kv = jnp.concatenate([w_k, w_v], axis=1)
        cosines, sines = rope_tables(positions, head)
        chunks = range(x_in.shape[0] // rep)

        def cut(arr, h):
            return arr[h * rep:(h + 1) * rep]

        def total(pieces):
            return functools.reduce(jnp.add, pieces)

        def mm(expr, left, right):
            return jnp.einsum(expr, left, right, preferred_element_type=F32)

        x_f32 = [cut(x_in, h).astype(F32) for h in chunks]
        normed, pre_pull, kv_proj, q_proj, kv_all, q_all = [], [], [], [], [], []
        for h in chunks:
            value, pull = jax.vjp(pre_norm, x_f32[h], w_pre)
            normed.append(value)
            pre_pull.append(pull)
            kv_proj.append(mm('bsd,dn->bsn', value, w_kv).astype(BF16))
            kv_all.append(exchange(kv_pack(kv_proj[h], k_norm, cosines, sines, head, kv_heads, rep)))
            q_proj.append(mm('bsd,dn->bsn', value, w_q).astype(BF16))
            q_all.append(exchange(q_pack(q_proj[h], q_norm, cosines, sines, head, kv_heads, rep)))
        fwd = [attention_fwd(q_all[h], kv_all[h], head) for h in chunks]
        y_out, dy_f32, d_oall, dw_o, dw_post = [], [], [], [], []
        for h in chunks:
            o_flat = unpack(exchange(fwd[h][0]), kv_heads, rep)
            proj = mm('bsn,nd->bsd', o_flat, w_o).astype(BF16)
            post, post_pull = jax.vjp(post_norm, proj, w_post)
            y_out.append((x_f32[h] + post).astype(BF16))
            dy_f32.append(cut(dy_in, h).astype(F32))
            d_proj, piece = post_pull(dy_f32[h])
            dw_post.append(piece)
            d_oall.append(exchange(pack(mm('bsd,nd->bsn', d_proj, w_o).astype(BF16), kv_heads, rep)))
            dw_o.append(mm('bsn,bsd->nd', o_flat, d_proj))
        dw_o = scatter(total(dw_o))
        d_all = []
        for h in chunks:
            if h == chunks[-1]:
                (d_oall[h], dw_o, *d_all) = lax.optimization_barrier((d_oall[h], dw_o, *d_all))
                dw_o = gather(dw_o)
            delta = row_dots(fwd[h][0], d_oall[h], head)
            d_all.append(attention_bwd(q_all[h], kv_all[h], d_oall[h], fwd[h][1], delta, head))
        d_all = [exchange(arr) for arr in d_all]
        dkv_parts, dq_parts, d_normed, dk_norm, dq_norm = [], [], [], [], []
        for h in chunks:
            if h == chunks[-1] and h > 0:
                d_all[h], dw_o, dkv_parts[-1], dq_parts[-1], d_normed[-1] = lax.optimization_barrier(
                    (d_all[h], dw_o, dkv_parts[-1], dq_parts[-1], d_normed[-1]))
            dk, dv, piece = kv_unpack(d_all[h], kv_proj[h], k_norm, cosines, sines, head, kv_heads, rep)
            dkv = jnp.concatenate([dk, dv], axis=-1)
            dk_norm.append(piece)
            dkv_parts.append(mm('bsd,bsn->dn', normed[h], dkv))
            dq, piece = q_unpack(d_all[h], q_proj[h], q_norm, cosines, sines, head, kv_heads, rep)
            dq_norm.append(piece)
            dq_parts.append(mm('bsd,bsn->dn', normed[h], dq))
            d_normed.append((mm('bsn,dn->bsd', dq, w_q) + mm('bsn,dn->bsd', dkv, w_kv)).astype(BF16))
        dw_kv = gather(scatter(total(dkv_parts)))
        dw_q = gather(scatter(total(dq_parts)))
        dx_out, dw_pre = [], []
        for h in chunks:
            dx_norm, piece = pre_pull[h](d_normed[h])
            dw_pre.append(piece)
            dx_out.append((dy_f32[h] + dx_norm).astype(BF16))
        y_out, dx_out = jnp.concatenate(y_out, axis=0), jnp.concatenate(dx_out, axis=0)
        dw_pre, dw_post, dq_norm, dk_norm = total(dw_pre), total(dw_post), total(dq_norm), total(dk_norm)
        small = lax.psum((dw_pre, dw_post, dq_norm.reshape(head), dk_norm.reshape(head)), 'sp')
        half = w_k.shape[1]
        return (y_out, dx_out, dw_q, dw_kv[:, :half], dw_kv[:, half:], dw_o, *small)

    token_spec = P('dp', 'sp', None)
    return jax.shard_map(device_step, mesh=mesh,
                         in_specs=(token_spec, token_spec, P(('dp', 'sp')), P(None, None), P(None, None), P(None, None), P(None, None), P(None), P(None), P(None), P(None)),
                         out_specs=(token_spec, token_spec, P('dp', None), P('dp', None), P('dp', None), P('dp', None), P('dp'), P('dp'), P('dp'), P('dp')),
                         check_vma=False)
```
